8 devices in a mesh: dp: 8 (over z, y, x, core).
Axes of the slice: x: 2, y: 2, z: 1, core: 2. Of those that a mesh axis runs over, the one named last changes fastest.
Arguments:
- x_in: bfloat16 [8192, 2048], P('dp')
- dy_mid: bfloat16 [8192, 5632], P('dp')
- x_mid: bfloat16 [8192, 5632], P('dp')
- dy_out: bfloat16 [8192, 2048], P('dp')
- w_fc1: float32 [2048, 5632], replicated
- w_fc2: float32 [5632, 2048], replicated
- stat_left: float32 [24, 1024, 1024], P('dp')
- stat_right: float32 [24, 1024, 1024], P('dp')
- root_left: float32 [24, 1024, 1024], P('dp')
- root_right: float32 [24, 1024, 1024], P('dp')
- graft_sq: float32 [24, 1024, 1024], P('dp')
- momentum: float32 [24, 1024, 1024], P('dp')
Outputs:
- output 1: float32 [2048, 5632], replicated
- output 2: float32 [5632, 2048], replicated
- output 3: float32 [24, 1024, 1024], P('dp')
- output 4: float32 [24, 1024, 1024], P('dp')
- output 5: float32 [24, 1024, 1024], P('dp')
- output 6: float32 [24, 1024, 1024], P('dp')
All inputs are finite; a program needn't handle non-finite values.
Results may differ from the reference program's by a relative error of at most 0.001.
Values are sent between devices in bfloat16 or wider.
A program may use at most 1.5 GiB of HBM per device.

```python
import jax
import jax.numpy as jnp

D = 2048
FF = 5632
BLOCK = 1024
TOKENS = 1024
DEVICES = 8
STEP = 10

ROW_BLOCKS = (D + BLOCK - 1) // BLOCK
COL_BLOCKS = (FF + BLOCK - 1) // BLOCK
HALF_BLOCKS = ROW_BLOCKS * COL_BLOCKS
NUM_BLOCKS = 2 * HALF_BLOCKS
ROWS_ALL = DEVICES * TOKENS
STAT_DECAY = 0.999
MOM_DECAY = 0.9
GRAFT_EPS = 1e-8
LEARN_RATE = 0.01
WEIGHT_DECAY = 1e-4
BIAS_CORR = 1.0 - STAT_DECAY ** STEP


def spd_draw(key_pair, low_diag, high_diag):
    diag_key, factor_key = jax.random.split(key_pair)
    diag_vals = jax.random.uniform(diag_key, (NUM_BLOCKS, BLOCK), jnp.float32, low_diag, high_diag)
    factor = jax.random.normal(factor_key, (NUM_BLOCKS, BLOCK, 64), jnp.float32)
    low_rank = jnp.einsum('nik,njk->nij', factor, factor) / 128.0
    return low_rank + diag_vals[:, :, None] * jnp.eye(BLOCK, dtype=jnp.float32)


def setup_inputs(seed: int = 0) -> dict:
    key_list = jax.random.split(jax.random.key(seed), 12)
    grad_scale = TOKENS ** -0.5
    stat_scale = 0.01 * BLOCK / DEVICES
    x_in = jax.random.normal(key_list[0], (ROWS_ALL, D), jnp.float32).astype(jnp.bfloat16)
    dy_mid = (jax.random.normal(key_list[1], (ROWS_ALL, FF), jnp.float32) * grad_scale).astype(jnp.bfloat16)
    x_mid = jax.random.normal(key_list[2], (ROWS_ALL, FF), jnp.float32).astype(jnp.bfloat16)
    dy_out = (jax.random.normal(key_list[3], (ROWS_ALL, D), jnp.float32) * grad_scale).astype(jnp.bfloat16)
    w_fc1 = jax.random.normal(key_list[4], (D, FF), jnp.float32) * D ** -0.5
    w_fc2 = jax.random.normal(key_list[5], (FF, D), jnp.float32) * FF ** -0.5
    stat_left = stat_scale * spd_draw(key_list[6], 0.2, 1.0)
    stat_right = stat_scale * spd_draw(key_list[7], 0.2, 1.0)
    root_left = spd_draw(key_list[8], 0.2, 1.0)
    root_right = spd_draw(key_list[9], 0.2, 1.0)
    graft_sq = (BIAS_CORR / DEVICES) * jax.random.uniform(key_list[10], (NUM_BLOCKS, BLOCK, BLOCK), jnp.float32, 0.2, 2.0)
    momentum = jax.random.normal(key_list[11], (NUM_BLOCKS, BLOCK, BLOCK), jnp.float32)
    return {'x_in': x_in, 'dy_mid': dy_mid, 'x_mid': x_mid, 'dy_out': dy_out, 'w_fc1': w_fc1, 'w_fc2': w_fc2, 'stat_left': stat_left, 'stat_right': stat_right, 'root_left': root_left, 'root_right': root_right, 'graft_sq': graft_sq, 'momentum': momentum}


def to_blocks(matrix, row_blocks, col_blocks):
    padded = jnp.pad(matrix, ((0, row_blocks * BLOCK - matrix.shape[0]), (0, col_blocks * BLOCK - matrix.shape[1])))
    return padded.reshape(row_blocks, BLOCK, col_blocks, BLOCK).transpose(0, 2, 1, 3).reshape(row_blocks * col_blocks, BLOCK, BLOCK)


def from_blocks(blocks, row_blocks, col_blocks, n_rows, n_cols):
    full_mat = blocks.reshape(row_blocks, col_blocks, BLOCK, BLOCK).transpose(0, 2, 1, 3)
    return full_mat.reshape(row_blocks * BLOCK, col_blocks * BLOCK)[:n_rows, :n_cols]


def keep_mask(block_ids):
    is_first = block_ids < HALF_BLOCKS
    local_ids = block_ids % HALF_BLOCKS
    row_first = jnp.minimum(D - (local_ids // COL_BLOCKS) * BLOCK, BLOCK)
    col_first = jnp.minimum(FF - (local_ids % COL_BLOCKS) * BLOCK, BLOCK)
    row_second = jnp.minimum(FF - (local_ids // ROW_BLOCKS) * BLOCK, BLOCK)
    col_second = jnp.minimum(D - (local_ids % ROW_BLOCKS) * BLOCK, BLOCK)
    row_count = jnp.where(is_first, row_first, row_second)
    col_count = jnp.where(is_first, col_first, col_second)
    offsets = jnp.arange(BLOCK)
    return (offsets[None, :, None] < row_count[:, None, None]) & (offsets[None, None, :] < col_count[:, None, None])


def reference(x_in, dy_mid, x_mid, dy_out, w_fc1, w_fc2, stat_left, stat_right, root_left, root_right, graft_sq, momentum):
    grad_fc1 = jnp.dot(x_in.T, dy_mid, preferred_element_type=jnp.float32) / DEVICES
    grad_fc2 = jnp.dot(x_mid.T, dy_out, preferred_element_type=jnp.float32) / DEVICES
    grad_blk = jnp.concatenate([to_blocks(grad_fc1, ROW_BLOCKS, COL_BLOCKS), to_blocks(grad_fc2, COL_BLOCKS, ROW_BLOCKS)], axis=0)
    new_left = STAT_DECAY * stat_left + (1.0 - STAT_DECAY) * jnp.einsum('nik,njk->nij', grad_blk, grad_blk)
    new_right = STAT_DECAY * stat_right + (1.0 - STAT_DECAY) * jnp.einsum('nki,nkj->nij', grad_blk, grad_blk)
    precond = jnp.einsum('nij,njk->nik', jnp.einsum('nij,njk->nik', root_left, grad_blk), root_right)
    precond = jnp.where(keep_mask(jnp.arange(NUM_BLOCKS)), precond, 0.0)
    new_sq = STAT_DECAY * graft_sq + (1.0 - STAT_DECAY) * grad_blk * grad_blk
    graft_dir = grad_blk / (jnp.sqrt(new_sq / BIAS_CORR) + GRAFT_EPS)
    graft_norm = jnp.sqrt(jnp.sum(graft_dir * graft_dir, axis=(1, 2)))
    pre_norm = jnp.sqrt(jnp.sum(precond * precond, axis=(1, 2)))
    new_mom = MOM_DECAY * momentum + precond * (graft_norm / pre_norm)[:, None, None]
    direction = new_mom.astype(jnp.bfloat16).astype(jnp.float32)
    dir_fc1 = from_blocks(direction[:HALF_BLOCKS], ROW_BLOCKS, COL_BLOCKS, D, FF)
    dir_fc2 = from_blocks(direction[HALF_BLOCKS:], COL_BLOCKS, ROW_BLOCKS, FF, D)
    new_w1 = w_fc1 - LEARN_RATE * (dir_fc1 + WEIGHT_DECAY * w_fc1)
    new_w2 = w_fc2 - LEARN_RATE * (dir_fc2 + WEIGHT_DECAY * w_fc2)
    return (new_w1, new_w2, new_left, new_right, new_sq, new_mom)
```

```python
import functools

import jax
import jax.numpy as jnp
from jax import lax
from jax.experimental import pallas as pl
from jax.experimental.pallas import tpu as pltpu
from jax.sharding import PartitionSpec as P

STEP = 10
STAT_DECAY = 0.999
MOM_DECAY = 0.9
GRAFT_EPS = 1e-8
LEARN_RATE = 0.01
WEIGHT_DECAY = 1e-4
BIAS_CORR = 1.0 - STAT_DECAY ** STEP


B = 1024
HALF = B // 2
LAST = 5
HBM = pltpu.HBM
ANY_SPEC = pl.BlockSpec(memory_space=HBM)
BF16 = jnp.bfloat16
F32 = jnp.float32
MIB = 1 << 20


def place():
    d = lax.axis_index("dp")
    return d // 4, (d // 2) % 2, d % 2


def tile_plan(kind, x, core):
    if kind == 0:
        return dict(p1=("s", 1 - x), p3=("s", x), p2=("l", 3 * core), p4=("l", 3 * core + 1), p5=("l", 3 * core + 2))
    far, own = 3 * (1 - x), 3 * x
    return dict(p1=("s", 0), p3=("s", 1), p2=("l", far + 2 * core), p4=("l", own + 2 * core),
                p5=("l", jnp.where(core == 0, far + 1, own + 1)))


def pack_body(specs, x_in, dy_mid, x_mid, dy_out, *rest):
    n = len(specs)
    outs, (buf, in_sem, out_sem) = rest[:n], rest[n:]
    depth = buf.shape[0]
    y, x, core = place()
    arrays = {(0, "s"): x_in, (0, "l"): dy_mid, (1, "s"): dy_out, (1, "l"): x_mid}

    def choices(spec):
        slot, target = spec
        for my_y in (0, 1):
            kind = 1 - my_y if target in ("send", "cross") else my_y
            c = 1 - core if target in ("cross", "sibling") else core
            form, tile = tile_plan(kind, x, c)[slot] if slot != "p5o" else tile_plan(kind, x, 1 - c)["p5"]
            yield y == my_y, arrays[kind, form], form, tile

    def load(i, wait):
        b = i % depth
        for cond, ref, form, tile in choices(specs[i]):
            def copy(h):
                cols = pl.ds(pl.multiple_of(tile * B + h * HALF, HALF), HALF)
                return pltpu.make_async_copy(ref.at[:, cols], buf.at[b, :, pl.ds(h * HALF, HALF)], in_sem.at[b, h])

            @pl.when(cond)
            def _():
                copy(0).wait() if wait else copy(0).start()

            full = cond if form == "s" else cond & (tile != LAST)

            @pl.when(full)
            def _():
                copy(1).wait() if wait else copy(1).start()

            if form == "l" and not wait:
                @pl.when(cond & (tile == LAST))
                def _():
                    @pl.loop(0, B // 64)
                    def _(r):
                        buf[b, pl.ds(r * 64, 64), HALF:] = jnp.zeros((64, HALF), BF16)

    def store(i):
        return pltpu.make_async_copy(buf.at[i % depth], outs[i], out_sem.at[i % depth])

    for i in range(min(depth - 1, n)):
        load(i, False)
    for i in range(n):
        load(i, True)
        store(i).start()
        j = i + depth - 1
        if j < n:
            if j - depth >= 0:
                store(j - depth).wait()
            load(j, False)
    for i in range(max(0, n - depth), n):
        store(i).wait()


def pack(specs, ins):
    n = len(specs)
    depth = min(4, n + 1)
    return pl.pallas_call(
        functools.partial(pack_body, specs),
        out_shape=[jax.ShapeDtypeStruct((B, B), BF16)] * n,
        in_specs=[ANY_SPEC] * 4,
        out_specs=[ANY_SPEC] * n,
        scratch_shapes=[pltpu.VMEM((depth, B, B), BF16), pltpu.SemaphoreType.DMA((depth, 2)),
                        pltpu.SemaphoreType.DMA((depth,))],
        cost_estimate=pl.CostEstimate(flops=n * 600_000_000, bytes_accessed=4 * n * MIB, transcendentals=0),
    )(*ins)


def mm_body(table, n_slots, *refs):
    slots = [refs[4 * i:4 * i + 4] for i in range(n_slots)]
    out, lhs, rhs, acc, lhs_sem, rhs_sem, out_sem = refs[4 * n_slots:]
    y, _, core = place()
    conds = (y == 0, (y == 1) & (core == 0), (y == 1) & (core == 1))

    for s in range(4):
        for cond, (a, b) in zip(conds, table):
            @pl.when(cond)
            def _():
                pltpu.make_async_copy(slots[a][s], lhs.at[s], lhs_sem.at[s]).start()
                pltpu.make_async_copy(slots[b][s], rhs.at[s], rhs_sem.at[s]).start()

    rows = 256
    chunks = B // rows

    def out_copy(m):
        at = pl.ds(pl.multiple_of(m * rows, rows), rows)
        return pltpu.make_async_copy(acc.at[at], out.at[at], out_sem.at[m])

    @pl.loop(0, 4)
    def _(s):
        pltpu.make_async_copy(slots[0][0], lhs.at[s], lhs_sem.at[s]).wait()
        pltpu.make_async_copy(slots[0][0], rhs.at[s], rhs_sem.at[s]).wait()

        @pl.loop(0, chunks)
        def _(m):
            at = pl.ds(pl.multiple_of(m * rows, rows), rows)
            part = lax.dot_general(lhs[s, :, at], rhs[s], (((0,), (0,)), ((), ())), preferred_element_type=F32)

            @pl.when(s == 0)
            def _():
                acc[at, :] = part

            @pl.when(s > 0)
            def _():
                acc[at, :] += part

            @pl.when(s == 3)
            def _():
                out_copy(m).start()

    for m in range(chunks):
        out_copy(m).wait()


def mm(table, slots):
    names = sorted({name for pair in table for name in pair})
    index = [tuple(names.index(name) for name in pair) for pair in table]
    args = [a for name in names for a in slots[name]]
    return pl.pallas_call(
        functools.partial(mm_body, index, len(names)),
        out_shape=jax.ShapeDtypeStruct((B, B), F32),
        in_specs=[ANY_SPEC] * len(args),
        out_specs=ANY_SPEC,
        scratch_shapes=[pltpu.VMEM((4, B, B), BF16), pltpu.VMEM((4, B, B), BF16), pltpu.VMEM((B, B), F32),
                        pltpu.SemaphoreType.DMA((4,)), pltpu.SemaphoreType.DMA((4,)), pltpu.SemaphoreType.DMA((4,))],
        cost_estimate=pl.CostEstimate(flops=8 * B * B * B, bytes_accessed=20 * MIB, transcendentals=0),
    )(*args)


def own_index(order):
    y, _, core = place()
    return jnp.where((y == 1) & (core == 1), (order + 1) % 3, order)


def split(v):
    hi = v.astype(BF16)
    return hi, (v - hi.astype(F32)).astype(BF16)


def fold(v):
    return jnp.sum(v.reshape(v.shape[0] // 8, 8, v.shape[1]), axis=0)


def dir_body(order, own, recv, root_l, root_r, graft, mom, *refs):
    if order > 0:
        refs = refs[2:]
    (g_out, sq_out, mom_out, da, db,
     gv, rv, lv, rrv, av, mv, gs, rs, ls, lgs, acc, dv, hsum, psum, sem_in, sem_out) = refs
    y, x, core = place()
    j = own_index(order)
    loads = [pltpu.make_async_copy(s, d, sem_in.at[i]) for i, (s, d) in enumerate(
        ((own, gv), (recv, rv), (root_r.at[j], rrv), (root_l.at[j], lv), (graft.at[j], av), (mom.at[j], mv)))]
    for c in loads:
        c.start()

    block = ((x * 2 + core) * 3) + j
    rows_first = jnp.int32(B)
    cols_first = jnp.where(block % 6 == LAST, HALF, B)
    rows_second = jnp.where(block // 2 == LAST, HALF, B)
    row_count = jnp.where(y == 0, rows_first, rows_second)
    col_count = jnp.where(y == 0, cols_first, B)

    hsum[...] = jnp.zeros_like(hsum)
    psum[...] = jnp.zeros_like(psum)
    loads[0].wait()
    loads[1].wait()
    step = 32

    @pl.loop(0, B // step)
    def _(r):
        at = pl.ds(pl.multiple_of(r * step, step), step)
        g = (gv[at, :] + rv[at, :]) * 0.125
        gv[at, :] = g
        gs[0, at, :], gs[1, at, :] = split(g)

    g_copy = pltpu.make_async_copy(gv, g_out, sem_out.at[0])
    g_copy.start()
    loads[2].wait()

    @pl.loop(0, B // step)
    def _(r):
        at = pl.ds(pl.multiple_of(r * step, step), step)
        rs[0, at, :], rs[1, at, :] = split(rrv[at, :])

    loads[3].wait()
    loads[4].wait()
    rows = 256

    def triple(a, b):
        acc[...] = jnp.zeros_like(acc)

        @pl.loop(0, 3)
        def _(p):
            acc[...] += jnp.dot(a[p // 2], b[p % 2], preferred_element_type=F32)

    @pl.loop(0, B // rows)
    def _(m):
        base = pl.multiple_of(m * rows, rows)

        @pl.loop(0, rows // step)
        def _(r):
            at = pl.ds(pl.multiple_of(r * step, step), step)
            ls[0, at, :], ls[1, at, :] = split(lv[pl.ds(base + r * step, step), :])

        triple(ls, gs)

        @pl.loop(0, rows // step)
        def _(r):
            at = pl.ds(pl.multiple_of(r * step, step), step)
            lgs[0, at, :], lgs[1, at, :] = split(acc[at, :])

        triple(lgs, rs)

        @pl.loop(0, rows // step)
        def _(r):
            at = pl.ds(pl.multiple_of(r * step, step), step)
            full = pl.ds(pl.multiple_of(base + r * step, step), step)
            row = lax.broadcasted_iota(jnp.int32, (step, B), 0) + (base + r * step)
            col = lax.broadcasted_iota(jnp.int32, (step, B), 1)
            p = jnp.where((row < row_count) & (col < col_count), acc[at, :], 0.0)
            rv[full, :] = p
            psum[...] += fold(p * p)
            g = gv[full, :]
            sq = STAT_DECAY * av[full, :] + (1.0 - STAT_DECAY) * g * g
            av[full, :] = sq
            h = g / (jnp.sqrt(sq / BIAS_CORR) + GRAFT_EPS)
            hsum[...] += fold(h * h)

    sq_copy = pltpu.make_async_copy(av, sq_out.at[j], sem_out.at[1])
    sq_copy.start()

    def total(v):
        return jnp.sum(jnp.sum(v[...], axis=0, keepdims=True), axis=1, keepdims=True)

    ratio = jnp.sqrt(total(hsum)) / jnp.sqrt(total(psum))
    loads[5].wait()

    @pl.loop(0, B // step)
    def _(r):
        at = pl.ds(pl.multiple_of(r * step, step), step)
        new = MOM_DECAY * mv[at, :] + rv[at, :] * ratio
        mv[at, :] = new
        dv[at, :] = new.astype(BF16)

    outs = [pltpu.make_async_copy(dv.at[pl.ds(0, HALF)], da, sem_out.at[2]),
            pltpu.make_async_copy(dv.at[pl.ds(HALF, HALF)], db, sem_out.at[3]),
            pltpu.make_async_copy(mv, mom_out.at[j], sem_out.at[4])]
    for c in outs:
        c.start()
    for c in [g_copy, sq_copy] + outs:
        c.wait()


def direction(order, own, recv, root_l, root_r, graft, mom, carried):
    tiles = jax.ShapeDtypeStruct((3, B, B), F32)
    args = [own, recv, root_l, root_r, graft, mom] + list(carried)
    full = pltpu.VMEM((B, B), F32)
    return pl.pallas_call(
        functools.partial(dir_body, order),
        out_shape=[jax.ShapeDtypeStruct((B, B), F32), tiles, tiles,
                   jax.ShapeDtypeStruct((HALF, B), BF16), jax.ShapeDtypeStruct((HALF, B), BF16)],
        in_specs=[ANY_SPEC] * len(args),
        out_specs=[ANY_SPEC] * 5,
        input_output_aliases={6: 1, 7: 2} if carried else {},
        scratch_shapes=[full] * 6 + [
            pltpu.VMEM((2, B, B), BF16), pltpu.VMEM((2, B, B), BF16), pltpu.VMEM((2, 256, B), BF16),
            pltpu.VMEM((2, 256, B), BF16), pltpu.VMEM((256, B), F32), pltpu.VMEM((B, B), BF16),
            pltpu.VMEM((8, B), F32), pltpu.VMEM((8, B), F32),
            pltpu.SemaphoreType.DMA((6,)), pltpu.SemaphoreType.DMA((5,))],
        compiler_params=pltpu.CompilerParams(vmem_limit_bytes=56 * MIB),
        cost_estimate=pl.CostEstimate(flops=12 * B * B * B, bytes_accessed=40 * MIB, transcendentals=3 * B * B),
    )(*args)


def stat_body(order, g, stat_l, stat_r, *refs):
    if order > 0:
        refs = refs[2:]
    l_out, r_out, gv, lv, rv, gs, acc, sem_in, sem_out = refs
    j = own_index(order)
    loads = [pltpu.make_async_copy(s, d, sem_in.at[i]) for i, (s, d) in enumerate(
        ((g, gv), (stat_l.at[j], lv), (stat_r.at[j], rv)))]
    for c in loads:
        c.start()
    step = 32
    loads[0].wait()

    @pl.loop(0, B // step)
    def _(r):
        at = pl.ds(pl.multiple_of(r * step, step), step)
        gs[0, at, :], gs[1, at, :] = split(gv[at, :])

    loads[1].wait()
    loads[2].wait()
    rows = 256

    def update(dst, base):
        @pl.loop(0, rows // step)
        def _(r):
            at = pl.ds(pl.multiple_of(r * step, step), step)
            full = pl.ds(pl.multiple_of(base + r * step, step), step)
            dst[full, :] = STAT_DECAY * dst[full, :] + (1.0 - STAT_DECAY) * acc[at, :]

    @pl.loop(0, B // rows)
    def _(m):
        base = pl.multiple_of(m * rows, rows)
        at = pl.ds(base, rows)
        acc[...] = jnp.zeros_like(acc)

        @pl.loop(0, 3)
        def _(p):
            acc[...] += lax.dot_general(gs[p // 2, at, :], gs[p % 2], (((1,), (1,)), ((), ())),
                                        preferred_element_type=F32)

        update(lv, base)
        acc[...] = jnp.zeros_like(acc)

        @pl.loop(0, 3)
        def _(p):
            acc[...] += lax.dot_general(gs[p // 2, :, at], gs[p % 2], (((0,), (0,)), ((), ())),
                                        preferred_element_type=F32)

        update(rv, base)

    outs = [pltpu.make_async_copy(lv, l_out.at[j], sem_out.at[0]),
            pltpu.make_async_copy(rv, r_out.at[j], sem_out.at[1])]
    for c in outs:
        c.start()
    for c in outs:
        c.wait()


def statistics(order, g, stat_l, stat_r, carried):
    tiles = jax.ShapeDtypeStruct((3, B, B), F32)
    args = [g, stat_l, stat_r] + list(carried)
    full = pltpu.VMEM((B, B), F32)
    return pl.pallas_call(
        functools.partial(stat_body, order),
        out_shape=[tiles, tiles],
        in_specs=[ANY_SPEC] * len(args),
        out_specs=[ANY_SPEC] * 2,
        input_output_aliases={3: 0, 4: 1} if carried else {},
        scratch_shapes=[full] * 3 + [pltpu.VMEM((2, B, B), BF16), pltpu.VMEM((256, B), F32),
                                     pltpu.SemaphoreType.DMA((3,)), pltpu.SemaphoreType.DMA((2,))],
        compiler_params=pltpu.CompilerParams(vmem_limit_bytes=48 * MIB),
        cost_estimate=pl.CostEstimate(flops=12 * B * B * B, bytes_accessed=20 * MIB, transcendentals=0),
    )(*args)


def weight_body(order, masks, w1, w2, *refs):
    n = 2 * len(masks)
    tiles = refs[:n]
    refs = refs[n + (2 if order > 0 else 0):]
    o1, o2, wv, dv, ov, sem_w, sem_d, sem_o = refs
    depth = wv.shape[0]
    me = lax.axis_index("dp")

    def cases(i):
        mask, half = masks[i // 2], i % 2
        dev = lax.bitwise_xor(me, jnp.int32(mask))
        first = dev < 4
        j = jnp.where(jnp.logical_not(first) & (dev % 2 == 1), (order + 1) % 3, order)
        block = jnp.where(first, 3 * dev + j, 3 * (dev - 4) + j)
        r1, c1, r2, c2 = block // 6, block % 6, block // 2, block % 2
        row1 = pl.multiple_of(r1 * B + half * HALF, HALF)
        row2 = pl.multiple_of(r2 * B + half * HALF, HALF)
        col1 = pl.multiple_of(c1 * B, HALF)
        col2 = pl.multiple_of(c2 * B, HALF)
        yield first & (c1 != LAST), w1, o1, row1, col1, B
        yield first & (c1 == LAST), w1, o1, row1, col1, HALF
        ok = jnp.logical_not(first) if half == 0 else jnp.logical_not(first) & (r2 != LAST)
        yield ok, w2, o2, row2, col2, B

    def act(i, what):
        b = i % depth
        for cond, w, o, row, col, width in cases(i):
            @pl.when(cond)
            def _():
                here = (pl.ds(row, HALF), pl.ds(col, width))
                into = (b, slice(None), pl.ds(0, width))
                if what in ("load", "wait"):
                    copy = pltpu.make_async_copy(w.at[here], wv.at[into], sem_w.at[b])
                else:
                    copy = pltpu.make_async_copy(ov.at[into], o.at[here], sem_o.at[b])
                copy.start() if what in ("load", "store") else copy.wait()
        if what in ("load", "wait"):
            copy = pltpu.make_async_copy(tiles[i], dv.at[b], sem_d.at[b])
            copy.start() if what == "load" else copy.wait()

    for i in range(depth - 1):
        act(i, "load")
    for i in range(n):
        b = i % depth
        act(i, "wait")
        if i >= depth:
            act(i - depth, "drain")

        @pl.loop(0, HALF // 32)
        def _(r):
            at = pl.ds(pl.multiple_of(r * 32, 32), 32)
            w = wv[b, at, :]
            ov[b, at, :] = w - LEARN_RATE * (dv[b, at, :].astype(F32) + WEIGHT_DECAY * w)

        act(i, "store")
        if i + depth - 1 < n:
            act(i + depth - 1, "load")
    for i in range(n - depth, n):
        act(i, "drain")


def weights(order, masks, w1, w2, tiles, carried):
    args = [w1, w2] + list(tiles) + list(carried)
    n = len(tiles)
    depth = 4
    return pl.pallas_call(
        functools.partial(weight_body, order, masks),
        out_shape=[jax.ShapeDtypeStruct(w1.shape, F32), jax.ShapeDtypeStruct(w2.shape, F32)],
        in_specs=[ANY_SPEC] * len(args),
        out_specs=[ANY_SPEC] * 2,
        input_output_aliases={n + 2: 0, n + 3: 1} if carried else {},
        scratch_shapes=[pltpu.VMEM((depth, HALF, B), F32), pltpu.VMEM((depth, HALF, B), BF16),
                        pltpu.VMEM((depth, HALF, B), F32), pltpu.SemaphoreType.DMA((depth,)),
                        pltpu.SemaphoreType.DMA((depth,)), pltpu.SemaphoreType.DMA((depth,))],
        cost_estimate=pl.CostEstimate(flops=20_000_000_000, bytes_accessed=80 * MIB, transcendentals=0),
    )(*args)


def solution(mesh):
    n_dev = mesh.shape["dp"]

    def hop(v, mask):
        return lax.ppermute(v, "dp", [(i, i ^ mask) for i in range(n_dev)])

    def per_device(x_in, dy_mid, x_mid, dy_out, w_fc1, w_fc2, stat_left, stat_right, root_left, root_right, graft_sq, momentum):
        ins = (x_in, dy_mid, x_mid, dy_out)
        p1, p2s, p2x = pack([("p1", "send"), ("p2", "send"), ("p2", "cross")], ins)
        r1, r2s, r2x = hop(p1, 4), hop(p2s, 4), hop(p2x, 5)
        p3, p4s, p4x, p5s, p5x = pack(
            [("p3", "send"), ("p4", "send"), ("p4", "cross"), ("p5", "send"), ("p5", "cross")], ins)
        r3, r4s, r4x, r5s, r5x = hop(p3, 4), hop(p4s, 4), hop(p4x, 5), hop(p5s, 4), hop(p5x, 5)
        names = ["p1", "p2", "p3", "p4", "p5", "p5o"]
        packed = pack([(s, "sibling") for s in names] + [(s, "own") for s in names], ins)
        sib = dict(zip(names, [hop(v, 1) for v in packed[:6]]))
        own = dict(zip(names, packed[6:]))
        slots = dict(
            p1=(own["p1"], sib["p1"], r1, hop(r1, 1)),
            p2=(own["p2"], sib["p2"], r2s, r2x),
            p3=(own["p3"], sib["p3"], r3, hop(r3, 1)),
            p4=(own["p4"], sib["p4"], r4s, r4x),
            p5=(own["p5"], sib["p5"], r5s, r5x),
            p5o=(own["p5o"], sib["p5o"], hop(r5x, 1), hop(r5s, 1)),
        )
        send_tables = ((("p1", "p2"), ("p2", "p1"), ("p2", "p1")),
                       (("p1", "p4"), ("p2", "p3"), ("p2", "p3")),
                       (("p1", "p5"), ("p5", "p1"), ("p5o", "p3")))
        own_tables = ((("p3", "p2"), ("p4", "p1"), ("p4", "p1")),
                      (("p3", "p4"), ("p4", "p3"), ("p4", "p3")),
                      (("p3", "p5"), ("p5o", "p1"), ("p5", "p3")))
        dirs, stats, wts = (), (), ()
        grads = []
        masks = (0, 4, 2, 6, 1, 5, 3, 7)
        for o in range(3):
            recv = hop(mm(send_tables[o], slots), 2)
            mine = mm(own_tables[o], slots)
            g, new_sq, new_mom, da, db = direction(o, mine, recv, root_left, root_right, graft_sq, momentum, dirs)
            dirs = (new_sq, new_mom)
            grads.append(g)
            a = {0: da, 4: hop(da, 4)}
            b = {0: db, 2: hop(db, 2)}
            a[2], a[6] = hop(a[0], 2), hop(a[4], 2)
            b[4], b[6] = hop(b[0], 4), hop(b[2], 4)
            for m in (0, 4, 2, 6):
                a[m + 1], b[m + 1] = hop(a[m], 1), hop(b[m], 1)
            tiles = [v for m in masks for v in (a[m], b[m])]
            wts = weights(o, masks, w_fc1, w_fc2, tiles, wts)
            stats = statistics(o, g, stat_left, stat_right, stats)
        return (*wts, *stats, *dirs)

    row_spec = P("dp", None)
    rep_spec = P(None, None)
    tile_spec = P("dp", None, None)
    in_specs = (row_spec,) * 4 + (rep_spec,) * 2 + (tile_spec,) * 6
    out_specs = (rep_spec,) * 2 + (tile_spec,) * 4
    return jax.shard_map(per_device, mesh=mesh, in_specs=in_specs, out_specs=out_specs, check_vma=False)
```

```python
import functools

import jax
import jax.numpy as jnp
from jax import lax
from jax.experimental import pallas as pl
from jax.experimental.pallas import tpu as pltpu
from jax.sharding import PartitionSpec as P


STEP = 10
STAT_DECAY = 0.999
MOM_DECAY = 0.9
GRAFT_EPS = 1e-8
LEARN_RATE = 0.01
WEIGHT_DECAY = 1e-4
BIAS_CORR = 1.0 - STAT_DECAY ** STEP


B = 1024
HALF = B // 2
LAST = 5
SLOTS = ["p1", "p2", "p3", "p4", "p5", "p6"]
HBM = pltpu.HBM
ANY_SPEC = pl.BlockSpec(memory_space=HBM)
BF16 = jnp.bfloat16
F32 = jnp.float32
MIB = 1 << 20
MESH = pl.DeviceIdType.MESH


def place():
    d = lax.axis_index("dp")
    return d // 4, (d // 2) % 2, d % 2


def tile_plan(kind, x, core):
    if kind == 0:
        return dict(p1=("s", 1 - x), p3=("s", x), p2=("l", 3 * core), p4=("l", 3 * core + 1), p5=("l", 3 * core + 2))
    far, own = 3 * (1 - x), 3 * x
    return dict(p1=("s", 0), p3=("s", 1), p2=("l", far + 2 * core), p4=("l", own + 2 * core),
                p5=("l", jnp.where(core == 0, far + 1, own + 1)))


def split(v):
    hi = v.astype(BF16)
    return hi, (v - hi.astype(F32)).astype(BF16)


def fold(v):
    return jnp.sum(v.reshape(v.shape[0] // 8, 8, v.shape[1]), axis=0)


def own_index(order):
    y, _, core = place()
    return jnp.where((y == 1) & (core == 1), (order + 1) % 3, order)


def each(n, step, f):
    @pl.loop(0, n // step)
    def _(r):
        f(pl.multiple_of(r * step, step))


def corners(ref):
    y, _, _ = place()
    for h in range(2):
        for q in range(2):
            yield y == 0, ref.at[pl.ds(q * HALF, HALF), pl.ds(h * HALF, HALF)], h, q
            yield y == 1, ref.at[pl.ds(h * HALF, HALF), pl.ds(q * HALF, HALF)], h, q


DIR_SCRATCH = [pltpu.VMEM((B, B), F32)] * 6 + [
    pltpu.VMEM((2, B, B), BF16), pltpu.VMEM((2, B, B), BF16), pltpu.VMEM((256, B), F32), pltpu.VMEM((B, B), BF16),
    pltpu.VMEM((8, B), F32), pltpu.VMEM((8, B), F32), pltpu.SemaphoreType.DMA((2, 2)), pltpu.SemaphoreType.DMA((4,)),
    pltpu.SemaphoreType.DMA((2,))]


def dir_loads(order, states, scr):
    root_l, root_r, graft, mom = states
    lv, rrv, av, mv, sem = scr[2], scr[3], scr[4], scr[5], scr[13]
    j = own_index(order)
    return [pltpu.make_async_copy(s.at[j], d, sem.at[i])
            for i, (s, d) in enumerate(((root_r, rrv), (root_l, lv), (graft, av), (mom, mv)))]


def dir_math(order, states, scr, g_out, mom_out, d_out):
    gv, rv, lv, rrv, av, mv, gs, rs, acc, dv, hsum, psum, sem_q, _, sem_out = scr
    loads = dir_loads(order, states, scr)
    y, x, core = place()
    block = ((x * 2 + core) * 3) + own_index(order)
    col_count = jnp.where((y == 0) & (block % 6 == LAST), HALF, B)
    row_count = jnp.where((y == 1) & (block // 2 == LAST), HALF, B)
    hsum[...] = jnp.zeros_like(hsum)
    psum[...] = jnp.zeros_like(psum)
    step = 64

    def make_grad(r):
        at = pl.ds(r, step)
        g = (gv[at, :] + rv[at, :]) * 0.125
        gv[at, :] = g
        gs[0, at, :], gs[1, at, :] = split(g)

    each(B, step, make_grad)
    g_copy = pltpu.make_async_copy(gv, g_out, sem_out.at[0])
    g_copy.start()
    loads[0].wait()

    def split_right(r):
        at = pl.ds(r, step)
        rs[0, at, :], rs[1, at, :] = split(rrv[at, :])

    each(B, step, split_right)
    loads[1].wait()
    loads[2].wait()
    rows = 256
    col = lax.broadcasted_iota(jnp.int32, (8, B), 1)

    def dot3(a_hi, a_lo, b):
        return (jnp.dot(a_hi, b[0], preferred_element_type=F32) + jnp.dot(a_hi, b[1], preferred_element_type=F32)
                + jnp.dot(a_lo, b[0], preferred_element_type=F32))

    @pl.loop(0, B // rows)
    def _(m):
        at = pl.ds(pl.multiple_of(m * rows, rows), rows)
        left = dot3(*split(lv[at, :]), gs)
        acc[...] = dot3(*split(left), rs)

        def finish(r):
            here = pl.ds(r, step)
            full = pl.ds(m * rows + r, step)
            kept = jnp.where(m * rows < row_count, col_count, 0)
            p = acc[here, :].reshape(step // 8, 8, B)
            p = jnp.where((col < kept)[None], p, 0.0)
            psum[...] += jnp.sum(p * p, axis=0)
            rv[full, :] = p.reshape(step, B)
            g = gv[full, :]
            sq = STAT_DECAY * av[full, :] + (1.0 - STAT_DECAY) * g * g
            h = g / (jnp.sqrt(sq * (1.0 / BIAS_CORR)) + GRAFT_EPS)
            hsum[...] += fold(h * h)

        each(rows, step, finish)

    def total(v):
        return jnp.sum(jnp.sum(v[...], axis=0, keepdims=True), axis=1, keepdims=True)

    ratio = jnp.sqrt(total(hsum)) / jnp.sqrt(total(psum))
    loads[3].wait()

    def momentum(r):
        at = pl.ds(r, step)
        new = MOM_DECAY * mv[at, :] + rv[at, :] * ratio
        mv[at, :] = new
        dv[at, :] = new.astype(BF16)

    each(B, step, momentum)
    mom_copy = pltpu.make_async_copy(mv, mom_out, sem_out.at[1])
    mom_copy.start()
    for cond, view, h, q in corners(dv):
        @pl.when(cond)
        def _():
            pltpu.make_async_copy(view, d_out.at[h, q], sem_q.at[h, q]).start()
    for h in range(2):
        for q in range(2):
            pltpu.make_async_copy(dv.at[pl.ds(0, HALF), pl.ds(0, HALF)], d_out.at[h, q], sem_q.at[h, q]).wait()
    return g_copy, mom_copy


def dir_body(order, own, recv, *refs):
    states, (g_out, mom_out, d_out), scr, sem_r = refs[:4], refs[4:7], refs[7:-1], refs[-1]
    gv, rv, sem_q = scr[0], scr[1], scr[12]
    for ref, src, sem in ((gv, own, sem_q), (rv, recv, sem_r)):
        for cond, view, h, q in corners(ref):
            @pl.when(cond)
            def _():
                pltpu.make_async_copy(src.at[h, q], view, sem.at[h, q]).start()
    for c in dir_loads(order, states, scr):
        c.start()
    for h in range(2):
        for q in range(2):
            for ref, src, sem in ((gv, own, sem_q), (rv, recv, sem_r)):
                pltpu.make_async_copy(src.at[h, q], ref.at[pl.ds(0, HALF), pl.ds(0, HALF)], sem.at[h, q]).wait()
    for c in dir_math(order, states, scr, g_out, mom_out, d_out):
        c.wait()


def direction(order, own, recv, states):
    tile = jax.ShapeDtypeStruct((B, B), F32)
    return pl.pallas_call(
        functools.partial(dir_body, order),
        out_shape=[tile, tile, jax.ShapeDtypeStruct((2, 2, HALF, HALF), BF16)],
        in_specs=[ANY_SPEC] * 6,
        out_specs=[ANY_SPEC] * 3,
        scratch_shapes=DIR_SCRATCH + [pltpu.SemaphoreType.DMA((2, 2))],
        compiler_params=pltpu.CompilerParams(vmem_limit_bytes=56 * MIB),
        cost_estimate=pl.CostEstimate(flops=12 * B * B * B, bytes_accessed=36 * MIB, transcendentals=3 * B * B),
    )(own, recv, *states)


Y_PIECES = [(n, h, t) for n, ts in (("p1", "s"), ("p2", "sx"), ("p3", "s"), ("p4", "sx"), ("p5", "sx")) for h in (0, 1) for t in ts]
RELAYS = [("p1", 0), ("p1", 1), ("p3", 0), ("p3", 1), ("s5", 0), ("x5", 0), ("s5", 1), ("x5", 1)]
SIBLINGS = [(n, h) for n in SLOTS for h in (0, 1)]
SENT = ((("p1", "p2"), ("p1", "p2"), ("p1", "p2")),
        (("p1", "p4"), ("p3", "p2"), ("p3", "p2")),
        (("p1", "p5"), ("p1", "p5"), ("p3", "p6")))
KEPT = ((("p3", "p2"), ("p1", "p4"), ("p1", "p4")),
        (("p3", "p4"), ("p3", "p4"), ("p3", "p4")),
        (("p3", "p5"), ("p1", "p6"), ("p3", "p5")))


def front_body(x_in, dy_mid, x_mid, dy_out, root_l, root_r, graft, mom,
               ry, rc, rsib, own2, recv2, g0, g1, mo0, mo1, d0, d1, dr0, xr,
               buf, xacc, y_send, y_recv, c_send, c_recv, s_send, s_recv, x_send, x_recv, d_send, d_recv,
               op_sem, r_sem, o_sem, *scr):
    states = (root_l, root_r, graft, mom)
    gv, rv = scr[0], scr[1]
    me = lax.axis_index("dp")
    y, x, core = place()
    roles = (y == 0, (y == 1) & (core == 0), (y == 1) & (core == 1))
    arrays = {(0, "s"): x_in, (0, "l"): dy_mid, (1, "s"): dy_out, (1, "l"): x_mid}
    first = y == 0

    def peer(mask):
        return lax.bitwise_xor(me, jnp.int32(mask))

    barrier = pltpu.get_barrier_semaphore()
    for mask in (1, 2, 4, 5):
        pl.semaphore_signal(barrier, inc=1, device_id=(peer(mask),), device_id_type=MESH)
    pl.semaphore_wait(barrier, 4)

    def plan(kind, c, name):
        return tile_plan(kind, x, 1 - c)["p5"] if name == "p6" else tile_plan(kind, x, c)[name]

    def view(kind, c, name, half):
        form, tile = plan(kind, c, name)
        cols = pl.ds(pl.multiple_of(tile * B + half * HALF, HALF), HALF)
        return arrays[kind, form].at[:, cols], tile != LAST if form == "l" and half else True

    def real(kind, c, name, half):
        form, tile = plan(kind, c, name)
        return tile != LAST if form == "l" and half else True

    def when(cond, f):
        if cond is True:
            f()
        else:
            pl.when(cond)(f)

    def both(*conds):
        out = True
        for c in conds:
            out = c if out is True else out if c is True else out & c
        return out


    def y_copy(i, src):
        mask = 4 if Y_PIECES[i][2] == "s" else 5
        return pltpu.make_async_remote_copy(src_ref=src, dst_ref=ry.at[i], send_sem=y_send.at[i], recv_sem=y_recv.at[i],
                                            device_id=(peer(mask),), device_id_type=MESH)

    def y_each(i, act):
        name, half, t = Y_PIECES[i]
        for my_y in (0, 1):
            src, ok = view(1 - my_y, core if t == "s" else 1 - core, name, half)
            when(both(y == my_y, ok), lambda: act(y_copy(i, src)))

    def y_arrive(name, half, t):
        i = Y_PIECES.index((name, half, t))
        for my_y in (0, 1):
            when(both(y == my_y, real(my_y, core, name, half)), lambda: y_copy(i, ry.at[i]).wait_recv())

    def sib_copy(k, src):
        return pltpu.make_async_remote_copy(src_ref=src, dst_ref=rsib.at[k], send_sem=s_send.at[k], recv_sem=s_recv.at[k],
                                            device_id=(peer(1),), device_id_type=MESH)

    def sib_each(k, act):
        name, half = SIBLINGS[k]
        for my_y in (0, 1):
            if name == "p6" and my_y == 0:
                continue
            src, ok = view(my_y, 1 - core, name, half)
            when(both(y == my_y, ok), lambda: act(sib_copy(k, src)))

    def sib_arrive(k):
        name, half = SIBLINGS[k]
        for my_y in (0, 1):
            if name == "p6" and my_y == 0:
                continue
            when(both(y == my_y, real(my_y, core, name, half)), lambda: sib_copy(k, rsib.at[k]).wait_recv())

    def relay(name, half):
        k = RELAYS.index((name, half))
        piece = (name, half, "s") if name[0] == "p" else ("p5", half, name[0])
        return pltpu.make_async_remote_copy(src_ref=ry.at[Y_PIECES.index(piece)], dst_ref=rc.at[k], send_sem=c_send.at[k],
                                            recv_sem=c_recv.at[k], device_id=(peer(1),), device_id_type=MESH)

    def relay_if(name):
        return True if name[0] == "p" else y == 1

    def x_real(order, half, d_core, d_x):
        if not half:
            return True
        ok1 = (y == 1) | (d_core == 0) if order == 2 else True
        ok2 = (y == 0) | (d_core == 0) | (d_x == 1) if order < 2 else True
        return both(ok1, ok2)

    def x_copy(order, half):
        dst = recv2.at[half] if order == 2 else xr.at[order, half]
        return pltpu.make_async_remote_copy(src_ref=xacc.at[half], dst_ref=dst, send_sem=x_send.at[order, half],
                                            recv_sem=x_recv.at[order, half], device_id=(peer(2),), device_id_type=MESH)

    def source(s, name, half):
        if s == 1:
            return rsib.at[SIBLINGS.index((name, half))]
        if name in ("p1", "p3"):
            return ry.at[Y_PIECES.index((name, half, "s"))] if s == 2 else rc.at[RELAYS.index((name, half))]
        if name == "p6":
            return rc.at[RELAYS.index(("x5" if s == 2 else "s5", half))]
        return ry.at[Y_PIECES.index((name, half, "s" if s == 2 else "x"))]


    def operand(s, table, part, halves, wait):
        for role, (cond, (short, long)) in enumerate(zip(roles, table)):
            name, half = (short, part) if part < 2 else (long, halves[part - 2])
            kind = min(role, 1)
            src = source(s, name, half) if s else view(kind, core, name, half)[0]

            def go():
                copy = pltpu.make_async_copy(src, buf.at[s, part], op_sem.at[s, part])
                copy.wait() if wait else copy.start()

            when(both(cond, real(kind, core, name, half)), go)

    def product(table, halves, arrivals, put, live):
        parts = range(2 + len(halves))
        for s in range(4):
            for part in parts:
                if (s, part) not in arrivals:
                    operand(s, table, part, halves, False)
        for s in range(4):
            for part in parts:
                if (s, part) in arrivals:
                    arrivals[s, part]()
                    operand(s, table, part, halves, False)
            for part in parts:
                operand(s, table, part, halves, True)
            for i, h in enumerate(halves):
                def dots():
                    @pl.loop(0, 2)
                    def _(q):
                        lhs = jnp.where(first, q, 2 + i)
                        rhs = jnp.where(first, 2 + i, q)
                        part = lax.dot_general(buf[s, lhs], buf[s, rhs], (((0,), (0,)), ((), ())),
                                               preferred_element_type=F32)
                        put(h, q, part, s == 0)

                when(live(h), dots)

    def put_sent(h, q, part, fresh):
        xacc[h, q] = part if fresh else xacc[h, q] + part

    def put_kept(h, q, part, fresh):
        rows = pl.ds(pl.multiple_of(jnp.where(first, q, h) * HALF, HALF), HALF)
        cols = pl.ds(pl.multiple_of(jnp.where(first, h, q) * HALF, HALF), HALF)
        gv[rows, cols] = part if fresh else gv[rows, cols] + part

    def send(order, half, arrivals):
        ok = x_real(order, half, core, x)
        if order:
            when(x_real(order - 1, half, core, x), lambda: x_copy(order - 1, half).wait_send())
        product(SENT[order], (half,), arrivals, put_sent, lambda h: ok)
        when(ok, lambda: x_copy(order, half).start())

    def keep(order):
        pads = [jnp.logical_not(jnp.asarray(x_real(order, 1, core, 1 - x)))]

        def clear(q):
            def zero(r):
                rows = pl.ds(pl.multiple_of(jnp.where(first, q, 1) * HALF, HALF) + r, 64)
                cols = pl.ds(pl.multiple_of(jnp.where(first, 1, q) * HALF, HALF), HALF)
                gv[rows, cols] = jnp.zeros((64, HALF), F32)

            each(HALF, 64, zero)

        @pl.when(pads[0])
        def _():
            clear(0)
            clear(1)

        product(KEPT[order], (0, 1), {}, put_kept, lambda h: True if h == 0 else x_real(order, 1, core, 1 - x))

    def take(order):
        for half in (0, 1):
            ok = x_real(order, half, core, 1 - x)
            when(ok, lambda: x_copy(order, half).wait_recv())
            for cond, spot, h, q in corners(rv):
                if h == half:
                    when(both(cond, ok), lambda: pltpu.make_async_copy(xr.at[order, h, q], spot, r_sem.at[h, q]).start())
            if half and ok is not True:
                for cond, spot, h, q in corners(rv):
                    if h == half:
                        def zero(r):
                            spot[pl.ds(r, 64), :] = jnp.zeros((64, HALF), F32)

                        when(both(cond, jnp.logical_not(ok)), lambda: each(HALF, 64, zero))
        for half in (0, 1):
            ok = x_real(order, half, core, 1 - x)
            for q in (0, 1):
                corner = rv.at[pl.ds(0, HALF), pl.ds(0, HALF)]
                when(ok, lambda: pltpu.make_async_copy(xr.at[order, half, q], corner, r_sem.at[half, q]).wait())


    for i in range(len(Y_PIECES)):
        y_each(i, lambda c: c.start())
    for k in range(len(SIBLINGS)):
        sib_each(k, lambda c: c.start())
    for c in dir_loads(0, states, scr):
        c.start()
    for k in range(len(SIBLINGS)):
        sib_arrive(k)
    for h in (0, 1):
        y_arrive("p1", h, "s")
        relay("p1", h).start()
    for h in (0, 1):
        relay("p1", h).wait_recv()
    for h in (0, 1):
        send(0, h, {(2, 2): lambda: y_arrive("p2", h, "s"), (3, 2): lambda: y_arrive("p2", h, "x")})
    for h in (0, 1):
        y_arrive("p3", h, "s")
        relay("p3", h).start()
    for h in (0, 1):
        relay("p3", h).wait_recv()
    for h in (0, 1):
        send(1, h, {(2, 2): lambda: y_arrive("p4", h, "s"), (3, 2): lambda: y_arrive("p4", h, "x")})
    keep(0)
    take(0)
    copies = dir_math(0, states, scr, g0, mo0, d0)
    to_y = pltpu.make_async_remote_copy(src_ref=d0, dst_ref=dr0, send_sem=d_send.at[0], recv_sem=d_recv.at[0],
                                        device_id=(peer(4),), device_id_type=MESH)
    to_y.start()

    def last_arrivals(h):
        for t in "sx":
            y_arrive("p5", h, t)
            when(y == 1, lambda: relay(t + "5", h).start())
        for t in "sx":
            when(y == 1, lambda: relay(t + "5", h).wait_recv())

    send(2, 0, {(2, 2): lambda: last_arrivals(0), (3, 2): lambda: None})
    for c in copies:
        c.wait()
    for c in dir_loads(1, states, scr):
        c.start()
    keep(1)
    take(1)
    copies = dir_math(1, states, scr, g1, mo1, d1)
    send(2, 1, {(2, 2): lambda: last_arrivals(1), (3, 2): lambda: None})
    for c in copies:
        c.wait()
    keep(2)
    for cond, spot, h, q in corners(gv):
        when(cond, lambda: pltpu.make_async_copy(spot, own2.at[h, q], o_sem.at[h, q]).start())
    for h in (0, 1):
        for q in (0, 1):
            pltpu.make_async_copy(gv.at[pl.ds(0, HALF), pl.ds(0, HALF)], own2.at[h, q], o_sem.at[h, q]).wait()
    pad = jnp.logical_not(jnp.asarray(x_real(2, 1, core, 1 - x)))

    @pl.when(pad)
    def _():
        def zero(r):
            rv[pl.ds(r, 64), :HALF] = jnp.zeros((64, HALF), F32)

        each(HALF, 64, zero)
        fill = [pltpu.make_async_copy(rv.at[pl.ds(0, HALF), pl.ds(0, HALF)], recv2.at[1, q], o_sem.at[0, q]) for q in (0, 1)]
        for c in fill:
            c.start()
        for c in fill:
            c.wait()

    for half in (0, 1):
        when(x_real(2, half, core, x), lambda: x_copy(2, half).wait_send())
        when(x_real(2, half, core, 1 - x), lambda: x_copy(2, half).wait_recv())
    to_y.wait()
    for i in range(len(Y_PIECES)):
        y_each(i, lambda c: c.wait_send())
    for k in range(len(SIBLINGS)):
        sib_each(k, lambda c: c.wait_send())
    for name, h in RELAYS:
        when(relay_if(name), lambda: relay(name, h).wait_send())


def front(ins, states):
    def tiles(*shape, dtype=F32):
        return jax.ShapeDtypeStruct(shape, dtype)

    dma = pltpu.SemaphoreType.DMA
    quarter = (2, 2, HALF, HALF)
    outs = [tiles(len(Y_PIECES), B, HALF, dtype=BF16), tiles(len(RELAYS), B, HALF, dtype=BF16),
            tiles(len(SIBLINGS), B, HALF, dtype=BF16), tiles(*quarter), tiles(*quarter), tiles(B, B), tiles(B, B),
            tiles(B, B), tiles(B, B), tiles(*quarter, dtype=BF16), tiles(*quarter, dtype=BF16), tiles(*quarter, dtype=BF16),
            tiles(2, *quarter)]
    res = pl.pallas_call(
        front_body,
        out_shape=outs,
        in_specs=[ANY_SPEC] * 8,
        out_specs=[ANY_SPEC] * len(outs),
        scratch_shapes=[pltpu.VMEM((4, 4, B, HALF), BF16), pltpu.VMEM(quarter, F32),
                        dma((16,)), dma((16,)), dma((8,)), dma((8,)), dma((12,)), dma((12,)), dma((3, 2)), dma((3, 2)),
                        dma((1,)), dma((1,)), dma((4, 4)), dma((2, 2)), dma((2, 2))] + DIR_SCRATCH,
        compiler_params=pltpu.CompilerParams(vmem_limit_bytes=67_000_000, collective_id=0, has_side_effects=True),
        cost_estimate=pl.CostEstimate(flops=200_000_000_000, bytes_accessed=400 * MIB, transcendentals=0),
    )(*ins, *states)
    return res[3:12]


def stat_body(order, g, mom, stat_l, stat_r, graft, *refs):
    if order > 0:
        refs = refs[4:]
    l_out, r_out, sq_out, mom_out, gv, lv, rv, av, mv, gs, sem_in, sem_out = refs
    j = own_index(order)
    loads = [pltpu.make_async_copy(s, d, sem_in.at[i]) for i, (s, d) in enumerate(
        ((g, gv), (stat_l.at[j], lv), (stat_r.at[j], rv), (graft.at[j], av), (mom, mv)))]
    for c in loads:
        c.start()
    outs = [pltpu.make_async_copy(s, d.at[j], sem_out.at[i]) for i, (s, d) in enumerate(
        ((lv, l_out), (rv, r_out), (av, sq_out), (mv, mom_out)))]
    loads[0].wait()
    loads[3].wait()

    def prepare(r):
        at = pl.ds(r, 64)
        g = gv[at, :]
        gs[0, at, :], gs[1, at, :] = split(g)
        av[at, :] = STAT_DECAY * av[at, :] + (1.0 - STAT_DECAY) * g * g

    each(B, 64, prepare)
    outs[2].start()
    loads[4].wait()
    outs[3].start()
    loads[1].wait()
    loads[2].wait()
    rows = 256

    def product(lhs_of, dims):
        def dot(a, b):
            return lax.dot_general(lhs_of(a), gs[b], (dims, ((), ())), preferred_element_type=F32)

        return dot(0, 0) + dot(0, 1) + dot(1, 0)

    @pl.loop(0, B // rows)
    def _(m):
        at = pl.ds(pl.multiple_of(m * rows, rows), rows)
        left = product(lambda a: gs[a, at, :], ((1,), (1,)))
        lv[at, :] = STAT_DECAY * lv[at, :] + (1.0 - STAT_DECAY) * left
        right = product(lambda a: gs[a, :, at], ((0,), (0,)))
        rv[at, :] = STAT_DECAY * rv[at, :] + (1.0 - STAT_DECAY) * right

    outs[0].start()
    outs[1].start()
    for c in outs:
        c.wait()


def statistics(order, g, mom, stat_l, stat_r, graft, carried):
    tiles = jax.ShapeDtypeStruct((3, B, B), F32)
    args = [g, mom, stat_l, stat_r, graft] + list(carried)
    full = pltpu.VMEM((B, B), F32)
    return pl.pallas_call(
        functools.partial(stat_body, order),
        out_shape=[tiles] * 4,
        in_specs=[ANY_SPEC] * len(args),
        out_specs=[ANY_SPEC] * 4,
        input_output_aliases={5 + i: i for i in range(4)} if carried else {},
        scratch_shapes=[full] * 5 + [pltpu.VMEM((2, B, B), BF16), pltpu.SemaphoreType.DMA((5,)), pltpu.SemaphoreType.DMA((4,))],
        compiler_params=pltpu.CompilerParams(vmem_limit_bytes=48 * MIB),
        cost_estimate=pl.CostEstimate(flops=12 * B * B * B, bytes_accessed=36 * MIB, transcendentals=0),
    )(*args)


def weight_body(order, pieces, w1, w2, *refs):
    n = len(pieces)
    tiles = refs[:n]
    o1, o2, wv, dv, ov, sem_w, sem_d, sem_o = refs[-8:]
    depth = wv.shape[0]
    me = lax.axis_index("dp")

    def cases(i, q):
        mask, half = pieces[i]
        dev = lax.bitwise_xor(me, jnp.int32(mask))
        first = dev < 4
        j = jnp.where(jnp.logical_not(first) & (dev % 2 == 1), (order + 1) % 3, order)
        block = jnp.where(first, 3 * dev + j, 3 * (dev - 4) + j)
        r1, c1, r2, c2 = block // 6, block % 6, block // 2, block % 2
        ok1, ok2 = first, jnp.logical_not(first)
        if half:
            ok1, ok2 = ok1 & (c1 != LAST), ok2 & (r2 != LAST)
        yield ok1, w1, o1, r1 * B + q * HALF, c1 * B + half * HALF
        yield ok2, w2, o2, r2 * B + half * HALF, c2 * B + q * HALF

    def act(i, what):
        b = i % depth
        for q in range(2):
            for cond, w, o, row, col in cases(i, q):
                @pl.when(cond)
                def _():
                    here = (pl.ds(pl.multiple_of(row, HALF), HALF), pl.ds(pl.multiple_of(col, HALF), HALF))
                    if what in ("load", "wait"):
                        copy = pltpu.make_async_copy(w.at[here], wv.at[b, q], sem_w.at[b, q])
                    else:
                        copy = pltpu.make_async_copy(ov.at[b, q], o.at[here], sem_o.at[b, q])
                    copy.start() if what in ("load", "store") else copy.wait()
        if what in ("load", "wait"):
            src = tiles[i] if len(tiles[i].shape) == 3 else tiles[i].at[pieces[i][1]]
            copy = pltpu.make_async_copy(src, dv.at[b], sem_d.at[b])
            copy.start() if what == "load" else copy.wait()

    for i in range(min(depth - 1, n)):
        act(i, "load")
    for i in range(n):
        b = i % depth
        act(i, "wait")
        if i >= depth:
            act(i - depth, "drain")

        @pl.loop(0, HALF // 32)
        def _(r):
            at = pl.ds(pl.multiple_of(r * 32, 32), 32)
            w = wv[b, :, at, :]
            ov[b, :, at, :] = w - LEARN_RATE * (dv[b, :, at, :].astype(F32) + WEIGHT_DECAY * w)

        act(i, "store")
        if i + depth - 1 < n:
            act(i + depth - 1, "load")
    for i in range(max(0, n - depth), n):
        act(i, "drain")


def weights(order, pieces, w1, w2, tiles, carried):
    args = [w1, w2] + list(tiles) + list(carried)
    n = len(tiles)
    depth = min(5, n)
    wide = pltpu.VMEM((depth, 2, HALF, HALF), F32)
    return pl.pallas_call(
        functools.partial(weight_body, order, pieces),
        out_shape=[jax.ShapeDtypeStruct(w1.shape, F32), jax.ShapeDtypeStruct(w2.shape, F32)],
        in_specs=[ANY_SPEC] * len(args),
        out_specs=[ANY_SPEC] * 2,
        input_output_aliases={n + 2: 0, n + 3: 1} if carried else {},
        scratch_shapes=[wide, pltpu.VMEM((depth, 2, HALF, HALF), BF16), wide, pltpu.SemaphoreType.DMA((depth, 2)),
                        pltpu.SemaphoreType.DMA((depth,)), pltpu.SemaphoreType.DMA((depth, 2))],
        cost_estimate=pl.CostEstimate(flops=n * 1_500_000_000, bytes_accessed=5 * n * MIB, transcendentals=0),
    )(*args)


def solution(mesh):
    n_dev = mesh.shape["dp"]

    def hop(v, mask):
        return lax.ppermute(v, "dp", [(i, i ^ mask) for i in range(n_dev)])

    def step(x_in, dy_mid, x_mid, dy_out, w_fc1, w_fc2, stat_left, stat_right, root_left, root_right, graft_sq, momentum):
        states = (root_left, root_right, graft_sq, momentum)
        own2, recv2, g0, g1, mo0, mo1, d0, d1, dr0 = front((x_in, dy_mid, x_mid, dy_out), states)
        g2, mo2, d2 = direction(2, own2, recv2, states)
        stats, wts = (), ()
        for o, (g, mo, d) in enumerate(((g0, mo0, d0), (g1, mo1, d1), (g2, mo2, d2))):
            stats = statistics(o, g, mo, stat_left, stat_right, graft_sq, stats)
            t = {0: d, 4: dr0 if o == 0 else hop(d, 4), 2: hop(d, 2)}
            t[6, 0] = hop(t[4][0], 2)
            t[6, 1] = hop(t[2][1], 4)
            for m in (0, 4, 2):
                t[m + 1] = hop(t[m], 1)
            for h in (0, 1):
                t[7, h] = hop(t[6, h], 1)

            def apply(masks, carried):
                pieces = [(m, h) for m in masks for h in (0, 1)]
                return weights(o, pieces, w_fc1, w_fc2, [t[m, h] if m > 5 else t[m] for m, h in pieces], carried)

            if o < 2:
                wts = apply((0, 4, 2, 6, 1, 5, 3, 7), wts)
            else:
                wts = apply((0, 1, 4, 5, 2, 3), wts)
                wts = apply((6, 7), wts)
        return (*wts, *stats)

    row_spec = P("dp", None)
    rep_spec = P(None, None)
    tile_spec = P("dp", None, None)
    in_specs = (row_spec,) * 4 + (rep_spec,) * 2 + (tile_spec,) * 6
    out_specs = (rep_spec,) * 2 + (tile_spec,) * 4
    return jax.shard_map(step, mesh=mesh, in_specs=in_specs, out_specs=out_specs, check_vma=False)
```
